16 devices in a mesh: rep: 4 (over y, z, core), dp: 4 (over x).
Axes of the slice: x: 4, y: 2, z: 1, core: 2. Of those that a mesh axis runs over, the one named last changes fastest.
The devices are a block of a 4x4x8 slice.
Arguments:
- a: bfloat16 [16, 4, 4096, 768], P(('rep', 'dp')), parts along dimension 0
- g: bfloat16 [16, 4, 4096, 3072], P(('rep', 'dp')), parts along dimension 0
Outputs:
- output: bfloat16 [16, 768, 3072], P('rep'), parts along dimension 0
There are 4 independent parts. The reference program is written for one: setup_inputs(seed, part) draws one part's arguments, and reference() takes and returns one part's arrays. A program takes and returns all parts, laid end to end along the dimension named above; each array names one.
All inputs are finite; a program needn't handle non-finite values.
Results may differ from the reference program's by a relative error of at most 0.012.
Values are sent between devices in bfloat16 or wider.
A program may use at most 768 MiB of HBM per device.

```python
import jax
import jax.numpy as jnp
from jax import lax

DEVICES = 4
MATRICES = 4
TOKENS = 4096
D = 768
FF = 3072


def setup_inputs(seed: int = 0, part: int = 0) -> dict:
    ka, kg, ks = (jax.random.fold_in(k, part) for k in jax.random.split(jax.random.key(seed), 3))
    size = 2.0 ** jax.random.uniform(ks, (DEVICES, MATRICES, 1, 1), jnp.float32, -1.0, 1.0)
    a = jax.random.normal(ka, (DEVICES, MATRICES, TOKENS, D), jnp.float32)
    g = size * jax.random.normal(kg, (DEVICES, MATRICES, TOKENS, FF), jnp.float32) * (DEVICES * TOKENS) ** -0.5
    return {"a": a.astype(jnp.bfloat16), "g": g.astype(jnp.bfloat16)}


def reference(a, g):
    def take(so_far, one):
        return so_far + jnp.einsum("ntd,ntf->ndf", *one, preferred_element_type=jnp.float32), None

    return lax.scan(take, jnp.zeros((MATRICES, D, FF), jnp.float32), (a, g))[0].astype(jnp.bfloat16)
```

```python
import functools

import jax
import jax.numpy as jnp
from jax import lax
from jax.experimental import pallas as pl
from jax.experimental.pallas import tpu as pltpu
from jax.sharding import PartitionSpec as P

COLS = 256
ROWS = 256
SLOTS = 3


def ring_kernel(ranks, a_hbm, g_hbm, sums, a_v, g_v, a_sem, g_sem, send_sem, recv_sem):
    mats, blocks, rows, _ = sums.shape
    per_mat = blocks // ranks
    units = mats * per_mat
    me = lax.axis_index("dp")
    right = lax.rem(me + 1, ranks)
    left = lax.rem(me + ranks - 1, ranks)

    def place(s, w):
        to_left = lax.rem(w, 2)
        b = lax.rem(me + (2 * ranks - s) + to_left * (2 * s), ranks)
        return w // per_mat, lax.rem(w, per_mat) * ranks + b

    def load_a(n):
        return pltpu.make_async_copy(a_hbm.at[0, n], a_v.at[n], a_sem.at[n])

    def load_g(i):
        n, c = place(i // units, lax.rem(i, units))
        slot = lax.rem(i, SLOTS)
        columns = pl.ds(pl.multiple_of(c * COLS, COLS), COLS)
        return pltpu.make_async_copy(g_hbm.at[0, n, :, columns], g_v.at[slot], g_sem.at[slot])

    def send(s, w, part):
        n, c = place(s, w)
        block = sums.at[n, c] if part is None else sums.at[n, c, part]
        to = right + lax.rem(w, 2) * (left - right)
        return pltpu.make_async_remote_copy(
            src_ref=block,
            dst_ref=block,
            send_sem=send_sem.at[s, w],
            recv_sem=recv_sem.at[s, w],
            device_id={"dp": to},
            device_id_type=pl.DeviceIdType.MESH,
        )

    def arrived(s, w):
        n, c = place(s + 1, w)
        pltpu.make_async_copy(sums.at[n, c], sums.at[n, c], recv_sem.at[s, w]).wait()

    def free(i):
        old = i - (ranks - 2) * units + 1

        @pl.when(jnp.logical_and(old >= 0, old < (ranks - 1) * units))
        def _():
            send(old // units, lax.rem(old, units), None).wait_send()

    load_a(0).start()
    load_g(0).start()
    load_g(1).start()
    for n in range(1, mats):
        load_a(n).start()

    barrier = pltpu.get_barrier_semaphore()
    for neighbour in (left, right):
        pl.semaphore_signal(barrier, inc=1, device_id={"dp": neighbour}, device_id_type=pl.DeviceIdType.MESH)
    pl.semaphore_wait(barrier, 2)

    def item(i, first):
        s, w = i // units, lax.rem(i, units)
        n, c = place(s, w)

        @pl.when(i + 2 < ranks * units)
        def _():
            load_g(i + 2).start()

        if first:

            @pl.when(lax.rem(w, per_mat) == 0)
            def _():
                load_a(n).wait()

        load_g(i).wait()
        if not first:
            arrived(s - 1, w)
            free(i)
        slot = lax.rem(i, SLOTS)
        for m in range(0, rows, ROWS):
            part = pl.ds(m, ROWS)
            term = lax.dot_general(
                a_v[n, :, m : m + ROWS],
                g_v[slot],
                (((0,), (0,)), ((), ())),
                preferred_element_type=jnp.float32,
            )
            if not first:
                term += sums[n, c, part].astype(jnp.float32)
            sums[n, c, part] = term.astype(sums.dtype)
            send(s, w, part).start()

    def first_item(i, carry):
        item(i, True)
        return carry

    def later_item(i, carry):
        item(i, False)
        return carry

    def forward(j, carry):
        s, w = j // units, lax.rem(j, units)
        arrived(s - 1, w)
        free(j)
        send(s, w, None).start()
        return carry

    def finish(j, carry):
        s, w = j // units, lax.rem(j, units)
        send(s, w, None).wait_send()
        return carry

    def last(w, carry):
        arrived(2 * ranks - 3, w)
        return carry

    lax.fori_loop(0, units, first_item, 0)
    lax.fori_loop(units, ranks * units, later_item, 0)
    lax.fori_loop(ranks * units, (2 * ranks - 2) * units, forward, 0)
    lax.fori_loop(0, units, last, 0)
    lax.fori_loop((ranks - 1) * units, (2 * ranks - 2) * units, finish, 0)


def write_kernel(sums, out, sem):
    mats, blocks = sums.shape[:2]

    def copy(n, c):
        return pltpu.make_async_copy(sums.at[n, c], out.at[n, :, pl.ds(c * COLS, COLS)], sem.at[n, c])

    for n in range(mats):
        for c in range(blocks):
            copy(n, c).start()
    for n in range(mats):
        for c in range(blocks):
            copy(n, c).wait()


def solution(mesh):
    ranks = mesh.shape["dp"]

    def local(a, g):
        _, mats, tokens, rows = a.shape
        width = g.shape[-1]
        blocks = width // COLS
        units = blocks // ranks * mats
        phases = 2 * ranks - 2
        sums = pl.pallas_call(
            functools.partial(ring_kernel, ranks),
            out_shape=pltpu.VMEM((mats, blocks, rows, COLS), jnp.bfloat16),
            in_specs=[pl.BlockSpec(memory_space=pltpu.HBM)] * 2,
            out_specs=pl.BlockSpec(memory_space=pltpu.VMEM),
            scratch_shapes=[
                pltpu.VMEM((mats, tokens, rows), jnp.bfloat16),
                pltpu.VMEM((SLOTS, tokens, COLS), jnp.bfloat16),
                pltpu.SemaphoreType.DMA((mats,)),
                pltpu.SemaphoreType.DMA((SLOTS,)),
                pltpu.SemaphoreType.DMA((phases, units)),
                pltpu.SemaphoreType.DMA((phases, units)),
            ],
            compiler_params=pltpu.CompilerParams(
                collective_id=0, has_side_effects=True, vmem_limit_bytes=42 * 2**20
            ),
            name="ring",
        )(a, g)
        return pl.pallas_call(
            write_kernel,
            out_shape=jax.ShapeDtypeStruct((mats, rows, width), jnp.bfloat16),
            in_specs=[pl.BlockSpec(memory_space=pltpu.VMEM)],
            out_specs=pl.BlockSpec(memory_space=pltpu.HBM),
            scratch_shapes=[pltpu.SemaphoreType.DMA((mats, blocks))],
            compiler_params=pltpu.CompilerParams(vmem_limit_bytes=2**20),
            name="write",
        )(pltpu.with_memory_space_constraint(sums, pltpu.VMEM))

    return jax.shard_map(
        local, mesh=mesh, in_specs=P(("rep", "dp")), out_specs=P("rep"), check_vma=False
    )
```

```python
import functools

import jax
import jax.numpy as jnp
from jax import lax
from jax.experimental import pallas as pl
from jax.experimental.pallas import tpu as pltpu
from jax.sharding import PartitionSpec as P

COLS = 256
ROWS = 256
FIRST = 128
TAIL, LAST = 8, 2
SLOTS = 4


def place(ranks, per_mat, me, s, w):
    to_left = lax.rem(w, 2)
    b = lax.rem(me + 2 * ranks - s + to_left * (2 * s), ranks)
    return w // per_mat, lax.rem(w, per_mat) * ranks + b


def kept(units):
    return units - TAIL + lax.rem(lax.axis_index("rep"), 2) * (TAIL - LAST)


def greet(ranks):
    me = lax.axis_index("dp")
    right = lax.rem(me + 1, ranks)
    left = lax.rem(me + ranks - 1, ranks)
    barrier = pltpu.get_barrier_semaphore()
    for neighbour in (left, right):
        pl.semaphore_signal(barrier, inc=1, device_id={"dp": neighbour}, device_id_type=pl.DeviceIdType.MESH)
    pl.semaphore_wait(barrier, 2)


def ring_kernel(ranks, a_hbm, g_hbm, sums, a_v, g_v, a_sem, a0_sem, g_sem, start_sem, send_sem, recv_sem):
    mats, blocks, rows, _ = sums.shape
    per_mat = blocks // ranks
    units = mats * per_mat
    me = lax.axis_index("dp")
    right = lax.rem(me + 1, ranks)
    left = lax.rem(me + ranks - 1, ranks)

    end = (2 * ranks - 3) * units + kept(units)

    def place_of(s, w):
        return place(ranks, per_mat, me, s, w)

    def load_a(n):
        return pltpu.make_async_copy(a_hbm.at[0, n], a_v.at[n], a_sem.at[n])

    cuts = [0, FIRST, *range(ROWS, rows + 1, ROWS)]
    tokens = a_v.shape[1]

    def load_a0(k):
        columns = pl.ds(cuts[k], cuts[k + 1] - cuts[k])
        return pltpu.make_async_copy(a_hbm.at[0, 0, :, columns], a_v.at[0, :, columns], a0_sem.at[k])

    def load_start(h):
        half = pl.ds(h * (tokens // 2), tokens // 2)
        copies = [(a_hbm.at[0, 0, half, pl.ds(0, FIRST)], a_v.at[0, half, pl.ds(0, FIRST)])]
        for i in range(2):
            n, c = place_of(0, i)
            columns = pl.ds(pl.multiple_of(c * COLS, COLS), COLS)
            copies.append((g_hbm.at[0, n, half, columns], g_v.at[half, pl.ds(i * COLS, COLS)]))
        return [pltpu.make_async_copy(*copy, start_sem.at[h, k]) for k, copy in enumerate(copies)]

    def slot(i):
        return pl.ds(pl.multiple_of(lax.rem(i, SLOTS) * COLS, COLS), COLS)

    def load_g(i):
        n, c = place_of(i // units, lax.rem(i, units))
        columns = pl.ds(pl.multiple_of(c * COLS, COLS), COLS)
        return pltpu.make_async_copy(g_hbm.at[0, n, :, columns], g_v.at[:, slot(i)], g_sem.at[lax.rem(i, SLOTS)])

    def send(s, w, part=()):
        n, c = place_of(s, w)
        block = sums.at[(n, c, *part)]
        to = right + lax.rem(w, 2) * (left - right)
        return pltpu.make_async_remote_copy(
            src_ref=block,
            dst_ref=block,
            send_sem=send_sem.at[s, w],
            recv_sem=recv_sem.at[s, w],
            device_id={"dp": to},
            device_id_type=pl.DeviceIdType.MESH,
        )

    def arrived(s, w):
        n, c = place_of(s + 1, w)
        pltpu.make_async_copy(sums.at[n, c], sums.at[n, c], recv_sem.at[s, w]).wait()

    def free(i):
        old = i - (ranks - 2) * units + 1

        @pl.when(jnp.logical_and(old >= 0, old < (ranks - 1) * units))
        def _():
            send(old // units, lax.rem(old, units)).wait_send()

    for h in range(2):
        for copy in load_start(h):
            copy.start()

    greet(ranks)

    def term_of(n, half, top, bottom, columns):
        return lax.dot_general(
            a_v[n, half, top:bottom],
            g_v[half, columns],
            (((0,), (0,)), ((), ())),
            preferred_element_type=jnp.float32,
        )

    both = slice(0, 2 * COLS)
    for k in range(len(cuts) - 1):
        part = pl.ds(cuts[k], cuts[k + 1] - cuts[k])
        if k == 0:
            term = 0.0
            for h in range(2):
                for copy in load_start(h):
                    copy.wait()
                if h == 0:
                    for later in range(1, len(cuts) - 1):
                        load_a0(later).start()
                    load_g(2).start()
                term += term_of(0, pl.ds(h * (tokens // 2), tokens // 2), 0, FIRST, both)
        else:
            load_a0(k).wait()
            term = term_of(0, slice(None), cuts[k], cuts[k + 1], both)
        for i in range(2):
            n, c = place_of(0, i)
            sums[n, c, part] = term[:, i * COLS : (i + 1) * COLS].astype(sums.dtype)
            send(0, i, (part,)).start()
        if k == 0:
            load_a(1).start()
            load_g(3).start()
    load_g(4).start()
    load_g(5).start()

    def item(i, first):
        s, w = i // units, lax.rem(i, units)
        n = w // per_mat

        if first:

            @pl.when(lax.rem(w, per_mat) == 0)
            def _():
                load_a(n).wait()

            @pl.when(jnp.logical_and(lax.rem(w, per_mat) == 0, n + 1 < mats))
            def _():
                load_a(n + 1).start()

        load_g(i).wait()
        if not first:
            arrived(s - 1, w)
            free(i)
        n, c = place_of(s, w)
        for top in range(0, rows, ROWS):
            part = pl.ds(top, ROWS)
            term = term_of(n, slice(None), top, top + ROWS, slot(i))
            if not first:
                term += sums[n, c, part].astype(jnp.float32)
            sums[n, c, part] = term.astype(sums.dtype)
            send(s, w, (part,)).start()

        @pl.when(i + SLOTS < ranks * units)
        def _():
            load_g(i + SLOTS).start()

    def first_item(i, carry):
        item(i, True)
        return carry

    def later_item(i, carry):
        item(i, False)
        return carry

    def forward(j, carry):
        s, w = j // units, lax.rem(j, units)
        arrived(s - 1, w)
        free(j)
        send(s, w).start()
        return carry

    def finish(j, carry):
        s, w = j // units, lax.rem(j, units)
        send(s, w).wait_send()
        return carry

    def last(j, carry):
        arrived(j // units, lax.rem(j, units))
        return carry

    lax.fori_loop(2, units, first_item, 0)
    lax.fori_loop(units, ranks * units, later_item, 0)
    lax.fori_loop(ranks * units, end, forward, 0)
    lax.fori_loop(end - units, end, last, 0)
    lax.fori_loop((ranks - 1) * units, end, finish, 0)


def tail_kernel(ranks, sums, written, tail, send_sem, recv_sem):
    del written
    mats, blocks = sums.shape[:2]
    per_mat = blocks // ranks
    units = mats * per_mat
    me = lax.axis_index("dp")
    right = lax.rem(me + 1, ranks)
    left = lax.rem(me + ranks - 1, ranks)

    def send(w):
        n, c = place(ranks, per_mat, me, 2 * ranks - 3, w)
        t = w - (units - TAIL)
        return pltpu.make_async_remote_copy(
            src_ref=sums.at[n, c],
            dst_ref=tail.at[t],
            send_sem=send_sem.at[t],
            recv_sem=recv_sem.at[t],
            device_id={"dp": right + lax.rem(w, 2) * (left - right)},
            device_id_type=pl.DeviceIdType.MESH,
        )

    def start(w, carry):
        send(w).start()
        return carry

    def finish(w, carry):
        send(w).wait()
        return carry

    greet(ranks)
    lax.fori_loop(kept(units), units, start, 0)
    lax.fori_loop(kept(units), units, finish, 0)


def write_kernel(ranks, sums, out, sem):
    mats, blocks = sums.shape[:2]
    per_mat = blocks // ranks
    units = mats * per_mat
    me = lax.axis_index("dp")

    def copies(act):
        for w in range(units):
            for s in range(ranks):
                n, c = place(ranks, per_mat, me, s, w)
                columns = pl.ds(pl.multiple_of(c * COLS, COLS), COLS)
                copy = pltpu.make_async_copy(sums.at[n, c], out.at[n, :, columns], sem.at[w, s])
                if s == ranks - 2 and w >= units - TAIL:
                    pl.when(w < kept(units))(functools.partial(act, copy))
                else:
                    act(copy)

    copies(lambda copy: copy.start())
    copies(lambda copy: copy.wait())


def rest_kernel(ranks, per_mat, units, written, tail, out, sem):
    del written
    me = lax.axis_index("dp")

    def copies(act):
        for t in range(TAIL):
            w = units - TAIL + t
            n, c = place(ranks, per_mat, me, ranks - 2, w)
            columns = pl.ds(pl.multiple_of(c * COLS, COLS), COLS)
            copy = pltpu.make_async_copy(tail.at[t], out.at[n, :, columns], sem.at[t])
            pl.when(w >= kept(units))(functools.partial(act, copy))

    copies(lambda copy: copy.start())
    copies(lambda copy: copy.wait())


def solution(mesh):
    ranks = mesh.shape["dp"]

    def local(a, g):
        _, mats, tokens, rows = a.shape
        width = g.shape[-1]
        blocks = width // COLS
        units = blocks // ranks * mats
        phases = 2 * ranks - 2
        sums = pl.pallas_call(
            functools.partial(ring_kernel, ranks),
            out_shape=pltpu.VMEM((mats, blocks, rows, COLS), jnp.bfloat16),
            in_specs=[pl.BlockSpec(memory_space=pltpu.HBM)] * 2,
            out_specs=pl.BlockSpec(memory_space=pltpu.VMEM),
            scratch_shapes=[
                pltpu.VMEM((mats, tokens, rows), jnp.bfloat16),
                pltpu.VMEM((tokens, SLOTS * COLS), jnp.bfloat16),
                pltpu.SemaphoreType.DMA((mats,)),
                pltpu.SemaphoreType.DMA((1 + rows // ROWS,)),
                pltpu.SemaphoreType.DMA((SLOTS,)),
                pltpu.SemaphoreType.DMA((2, 3)),
                pltpu.SemaphoreType.DMA((phases, units)),
                pltpu.SemaphoreType.DMA((phases, units)),
            ],
            compiler_params=pltpu.CompilerParams(
                collective_id=0, has_side_effects=True, vmem_limit_bytes=44 * 2**20
            ),
            name="ring",
        )(a, g)
        sums = pltpu.with_memory_space_constraint(sums, pltpu.VMEM)
        hbm, vmem = pl.BlockSpec(memory_space=pltpu.HBM), pl.BlockSpec(memory_space=pltpu.VMEM)
        whole = jax.ShapeDtypeStruct((mats, rows, width), jnp.bfloat16)
        written = pl.pallas_call(
            functools.partial(write_kernel, ranks),
            out_shape=whole,
            in_specs=[vmem],
            out_specs=hbm,
            scratch_shapes=[pltpu.SemaphoreType.DMA((units, ranks))],
            compiler_params=pltpu.CompilerParams(vmem_limit_bytes=2**20),
            name="write",
        )(sums)
        tail = pl.pallas_call(
            functools.partial(tail_kernel, ranks),
            out_shape=pltpu.VMEM((TAIL, rows, COLS), jnp.bfloat16),
            in_specs=[vmem, hbm],
            out_specs=vmem,
            scratch_shapes=[pltpu.SemaphoreType.DMA((TAIL,))] * 2,
            compiler_params=pltpu.CompilerParams(
                collective_id=1, has_side_effects=True, vmem_limit_bytes=2**20
            ),
            name="tail",
        )(sums, pltpu.with_memory_space_constraint(written, pltpu.HBM))
        return pl.pallas_call(
            functools.partial(rest_kernel, ranks, blocks // ranks, units),
            out_shape=whole,
            in_specs=[hbm, vmem],
            out_specs=hbm,
            input_output_aliases={0: 0},
            scratch_shapes=[pltpu.SemaphoreType.DMA((TAIL,))],
            compiler_params=pltpu.CompilerParams(vmem_limit_bytes=2**20),
            name="rest",
        )(written, pltpu.with_memory_space_constraint(tail, pltpu.VMEM))

    return jax.shard_map(
        local, mesh=mesh, in_specs=P(("rep", "dp")), out_specs=P("rep"), check_vma=False
    )
```

```python
import functools

import jax
import jax.numpy as jnp
from jax import lax
from jax.experimental import pallas as pl
from jax.experimental.pallas import tpu as pltpu
from jax.sharding import PartitionSpec as P

COLS = 256
ROWS = 256
FIRST = 128
TAIL, LAST = 8, 2
SLOTS = 4


def place(ranks, per_mat, me, s, w):
    to_left = lax.rem(w, 2)
    b = lax.rem(me + 2 * ranks - s + to_left * (2 * s), ranks)
    return w // per_mat, lax.rem(w, per_mat) * ranks + b


def kept(units):
    return units - LAST - lax.rem(lax.axis_index("rep"), 2) * (TAIL - LAST)


def greet(ranks):
    me = lax.axis_index("dp")
    right = lax.rem(me + 1, ranks)
    left = lax.rem(me + ranks - 1, ranks)
    barrier = pltpu.get_barrier_semaphore()
    for neighbour in (left, right):
        pl.semaphore_signal(barrier, inc=1, device_id={"dp": neighbour}, device_id_type=pl.DeviceIdType.MESH)
    pl.semaphore_wait(barrier, 2)


def ring_kernel(ranks, a_hbm, g_hbm, sums, a_v, g_v, a_sem, a0_sem, g_sem, start_sem, send_sem, recv_sem):
    mats, blocks, rows, _ = sums.shape
    per_mat = blocks // ranks
    units = mats * per_mat
    me = lax.axis_index("dp")
    right = lax.rem(me + 1, ranks)
    left = lax.rem(me + ranks - 1, ranks)

    end = (2 * ranks - 3) * units + kept(units)

    def place_of(s, w):
        return place(ranks, per_mat, me, s, w)

    def load_a(n):
        return pltpu.make_async_copy(a_hbm.at[0, n], a_v.at[n], a_sem.at[n])

    cuts = [0, FIRST, *range(ROWS, rows + 1, ROWS)]
    tokens = a_v.shape[1]

    def load_a0(k):
        columns = pl.ds(cuts[k], cuts[k + 1] - cuts[k])
        return pltpu.make_async_copy(a_hbm.at[0, 0, :, columns], a_v.at[0, :, columns], a0_sem.at[k])

    def load_start(h):
        half = pl.ds(h * (tokens // 2), tokens // 2)
        copies = [(a_hbm.at[0, 0, half, pl.ds(0, FIRST)], a_v.at[0, half, pl.ds(0, FIRST)])]
        for i in range(2):
            n, c = place_of(0, i)
            columns = pl.ds(pl.multiple_of(c * COLS, COLS), COLS)
            copies.append((g_hbm.at[0, n, half, columns], g_v.at[half, pl.ds(i * COLS, COLS)]))
        return [pltpu.make_async_copy(*copy, start_sem.at[h, k]) for k, copy in enumerate(copies)]

    def slot(i):
        return pl.ds(pl.multiple_of(lax.rem(i, SLOTS) * COLS, COLS), COLS)

    def load_g(i):
        n, c = place_of(i // units, lax.rem(i, units))
        columns = pl.ds(pl.multiple_of(c * COLS, COLS), COLS)
        return pltpu.make_async_copy(g_hbm.at[0, n, :, columns], g_v.at[:, slot(i)], g_sem.at[lax.rem(i, SLOTS)])

    def send(s, w, part=()):
        n, c = place_of(s, w)
        block = sums.at[(n, c, *part)]
        to = right + lax.rem(w, 2) * (left - right)
        return pltpu.make_async_remote_copy(
            src_ref=block,
            dst_ref=block,
            send_sem=send_sem.at[s, w],
            recv_sem=recv_sem.at[s, w],
            device_id={"dp": to},
            device_id_type=pl.DeviceIdType.MESH,
        )

    def arrived(s, w):
        n, c = place_of(s + 1, w)
        pltpu.make_async_copy(sums.at[n, c], sums.at[n, c], recv_sem.at[s, w]).wait()

    def free(i):
        old = i - (ranks - 2) * units + 1

        @pl.when(jnp.logical_and(old >= 0, old < (ranks - 1) * units))
        def _():
            send(old // units, lax.rem(old, units)).wait_send()

    for h in range(2):
        for copy in load_start(h):
            copy.start()

    greet(ranks)

    def term_of(n, half, top, bottom, columns):
        return lax.dot_general(
            a_v[n, half, top:bottom],
            g_v[half, columns],
            (((0,), (0,)), ((), ())),
            preferred_element_type=jnp.float32,
        )

    both = slice(0, 2 * COLS)
    for k in range(len(cuts) - 1):
        part = pl.ds(cuts[k], cuts[k + 1] - cuts[k])
        if k == 0:
            term = 0.0
            for h in range(2):
                for copy in load_start(h):
                    copy.wait()
                if h == 0:
                    for later in range(1, len(cuts) - 1):
                        load_a0(later).start()
                    load_g(2).start()
                term += term_of(0, pl.ds(h * (tokens // 2), tokens // 2), 0, FIRST, both)
        else:
            load_a0(k).wait()
            term = term_of(0, slice(None), cuts[k], cuts[k + 1], both)
        for i in range(2):
            n, c = place_of(0, i)
            sums[n, c, part] = term[:, i * COLS : (i + 1) * COLS].astype(sums.dtype)
            send(0, i, (part,)).start()
        if k == 0:
            load_a(1).start()
            load_g(3).start()
    load_g(4).start()
    load_g(5).start()

    def item(i, first):
        s, w = i // units, lax.rem(i, units)
        n = w // per_mat

        if first:

            @pl.when(lax.rem(w, per_mat) == 0)
            def _():
                load_a(n).wait()

            @pl.when(jnp.logical_and(lax.rem(w, per_mat) == 0, n + 1 < mats))
            def _():
                load_a(n + 1).start()

        load_g(i).wait()
        if not first:
            arrived(s - 1, w)
            free(i)
        n, c = place_of(s, w)
        for top in range(0, rows, ROWS):
            part = pl.ds(top, ROWS)
            term = term_of(n, slice(None), top, top + ROWS, slot(i))
            if not first:
                term += sums[n, c, part].astype(jnp.float32)
            sums[n, c, part] = term.astype(sums.dtype)
            send(s, w, (part,)).start()

        @pl.when(i + SLOTS < ranks * units)
        def _():
            load_g(i + SLOTS).start()

    def first_item(i, carry):
        item(i, True)
        return carry

    def later_item(i, carry):
        item(i, False)
        return carry

    def forward(j, carry):
        s, w = j // units, lax.rem(j, units)
        arrived(s - 1, w)
        free(j)
        send(s, w).start()
        return carry

    def finish(j, carry):
        s, w = j // units, lax.rem(j, units)
        send(s, w).wait_send()
        return carry

    def last(j, carry):
        arrived(j // units, lax.rem(j, units))
        return carry

    lax.fori_loop(2, units, first_item, 0)
    lax.fori_loop(units, ranks * units, later_item, 0)
    lax.fori_loop(ranks * units, end, forward, 0)
    lax.fori_loop(end - units, end, last, 0)
    lax.fori_loop((ranks - 1) * units, end, finish, 0)


def tail_kernel(ranks, sums, written, tail, send_sem, recv_sem):
    del written
    mats, blocks = sums.shape[:2]
    per_mat = blocks // ranks
    units = mats * per_mat
    me = lax.axis_index("dp")
    right = lax.rem(me + 1, ranks)
    left = lax.rem(me + ranks - 1, ranks)

    def send(w):
        n, c = place(ranks, per_mat, me, 2 * ranks - 3, w)
        t = w - (units - TAIL)
        return pltpu.make_async_remote_copy(
            src_ref=sums.at[n, c],
            dst_ref=tail.at[t],
            send_sem=send_sem.at[t],
            recv_sem=recv_sem.at[t],
            device_id={"dp": right + lax.rem(w, 2) * (left - right)},
            device_id_type=pl.DeviceIdType.MESH,
        )

    def start(w, carry):
        send(w).start()
        return carry

    def finish(w, carry):
        send(w).wait()
        return carry

    greet(ranks)
    lax.fori_loop(kept(units), units, start, 0)
    lax.fori_loop(kept(units), units, finish, 0)


def write_kernel(ranks, sums, out, sem):
    mats, blocks = sums.shape[:2]
    per_mat = blocks // ranks
    units = mats * per_mat
    me = lax.axis_index("dp")

    def copies(act):
        for w in range(units):
            for s in range(ranks):
                n, c = place(ranks, per_mat, me, s, w)
                columns = pl.ds(pl.multiple_of(c * COLS, COLS), COLS)
                copy = pltpu.make_async_copy(sums.at[n, c], out.at[n, :, columns], sem.at[w, s])
                if s == ranks - 2 and w >= units - TAIL:
                    pl.when(w < kept(units))(functools.partial(act, copy))
                else:
                    act(copy)

    copies(lambda copy: copy.start())
    copies(lambda copy: copy.wait())


def rest_kernel(ranks, per_mat, units, written, tail, out, sem):
    del written
    me = lax.axis_index("dp")

    def copies(act):
        for t in range(TAIL):
            w = units - TAIL + t
            n, c = place(ranks, per_mat, me, ranks - 2, w)
            columns = pl.ds(pl.multiple_of(c * COLS, COLS), COLS)
            copy = pltpu.make_async_copy(tail.at[t], out.at[n, :, columns], sem.at[t])
            pl.when(w >= kept(units))(functools.partial(act, copy))

    copies(lambda copy: copy.start())
    copies(lambda copy: copy.wait())


def solution(mesh):
    ranks = mesh.shape["dp"]

    def local(a, g):
        _, mats, tokens, rows = a.shape
        width = g.shape[-1]
        blocks = width // COLS
        units = blocks // ranks * mats
        phases = 2 * ranks - 2
        sums = pl.pallas_call(
            functools.partial(ring_kernel, ranks),
            out_shape=pltpu.VMEM((mats, blocks, rows, COLS), jnp.bfloat16),
            in_specs=[pl.BlockSpec(memory_space=pltpu.HBM)] * 2,
            out_specs=pl.BlockSpec(memory_space=pltpu.VMEM),
            scratch_shapes=[
                pltpu.VMEM((mats, tokens, rows), jnp.bfloat16),
                pltpu.VMEM((tokens, SLOTS * COLS), jnp.bfloat16),
                pltpu.SemaphoreType.DMA((mats,)),
                pltpu.SemaphoreType.DMA((1 + rows // ROWS,)),
                pltpu.SemaphoreType.DMA((SLOTS,)),
                pltpu.SemaphoreType.DMA((2, 3)),
                pltpu.SemaphoreType.DMA((phases, units)),
                pltpu.SemaphoreType.DMA((phases, units)),
            ],
            compiler_params=pltpu.CompilerParams(
                collective_id=0, has_side_effects=True, vmem_limit_bytes=44 * 2**20
            ),
            name="ring",
        )(a, g)
        sums = pltpu.with_memory_space_constraint(sums, pltpu.VMEM)
        hbm, vmem = pl.BlockSpec(memory_space=pltpu.HBM), pl.BlockSpec(memory_space=pltpu.VMEM)
        whole = jax.ShapeDtypeStruct((mats, rows, width), jnp.bfloat16)
        written = pl.pallas_call(
            functools.partial(write_kernel, ranks),
            out_shape=whole,
            in_specs=[vmem],
            out_specs=hbm,
            scratch_shapes=[pltpu.SemaphoreType.DMA((units, ranks))],
            compiler_params=pltpu.CompilerParams(vmem_limit_bytes=2**20),
            name="write",
        )(sums)
        tail = pl.pallas_call(
            functools.partial(tail_kernel, ranks),
            out_shape=pltpu.VMEM((TAIL, rows, COLS), jnp.bfloat16),
            in_specs=[vmem, hbm],
            out_specs=vmem,
            scratch_shapes=[pltpu.SemaphoreType.DMA((TAIL,))] * 2,
            compiler_params=pltpu.CompilerParams(
                collective_id=1, has_side_effects=True, vmem_limit_bytes=2**20
            ),
            name="tail",
        )(sums, pltpu.with_memory_space_constraint(written, pltpu.HBM))
        return pl.pallas_call(
            functools.partial(rest_kernel, ranks, blocks // ranks, units),
            out_shape=whole,
            in_specs=[hbm, vmem],
            out_specs=hbm,
            input_output_aliases={0: 0},
            scratch_shapes=[pltpu.SemaphoreType.DMA((TAIL,))],
            compiler_params=pltpu.CompilerParams(vmem_limit_bytes=2**20),
            name="rest",
        )(written, pltpu.with_memory_space_constraint(tail, pltpu.VMEM))

    return jax.shard_map(
        local, mesh=mesh, in_specs=P(("rep", "dp")), out_specs=P("rep"), check_vma=False
    )
```

```python
import functools

import jax
import jax.numpy as jnp
from jax import lax
from jax.experimental import pallas as pl
from jax.experimental.pallas import tpu as pltpu
from jax.sharding import PartitionSpec as P

COLS = 256
ROWS = 256
FIRST = 128
SHARES = 8
TAIL, LAST = 8, 2
SLOTS = 4


def place(ranks, per_mat, me, s, w):
    to_left = lax.rem(w, 2)
    b = lax.rem(me + 2 * ranks - s + to_left * (2 * s), ranks)
    return w // per_mat, lax.rem(w, per_mat) * ranks + b


def kept(units):
    return units - LAST - lax.rem(lax.axis_index("rep"), 2) * (TAIL - LAST)


def greet(ranks):
    me = lax.axis_index("dp")
    right = lax.rem(me + 1, ranks)
    left = lax.rem(me + ranks - 1, ranks)
    barrier = pltpu.get_barrier_semaphore()
    for neighbour in (left, right):
        pl.semaphore_signal(barrier, inc=1, device_id={"dp": neighbour}, device_id_type=pl.DeviceIdType.MESH)
    pl.semaphore_wait(barrier, 2)


def ring_kernel(ranks, a_hbm, g_hbm, sums, a_v, g_v, a_sem, a0_sem, g_sem, start_sem, send_sem, recv_sem):
    mats, blocks, rows, _ = sums.shape
    per_mat = blocks // ranks
    units = mats * per_mat
    me = lax.axis_index("dp")
    right = lax.rem(me + 1, ranks)
    left = lax.rem(me + ranks - 1, ranks)

    end = (2 * ranks - 3) * units + kept(units)

    def place_of(s, w):
        return place(ranks, per_mat, me, s, w)

    def load_a(n):
        return pltpu.make_async_copy(a_hbm.at[0, n], a_v.at[n], a_sem.at[n])

    cuts = [0, FIRST, *range(ROWS, rows + 1, ROWS)]
    tokens = a_v.shape[1]

    def load_a0(k):
        columns = pl.ds(cuts[k], cuts[k + 1] - cuts[k])
        return pltpu.make_async_copy(a_hbm.at[0, 0, :, columns], a_v.at[0, :, columns], a0_sem.at[k])

    def share(h):
        return pl.ds(h * (tokens // SHARES), tokens // SHARES)

    def load_start(h):
        some = share(h)
        copies = [(a_hbm.at[0, 0, some, pl.ds(0, FIRST)], a_v.at[0, some, pl.ds(0, FIRST)])]
        for i in range(2):
            n, c = place_of(0, i)
            columns = pl.ds(pl.multiple_of(c * COLS, COLS), COLS)
            copies.append((g_hbm.at[0, n, some, columns], g_v.at[some, pl.ds(i * COLS, COLS)]))
        return [pltpu.make_async_copy(*copy, start_sem.at[h, k]) for k, copy in enumerate(copies)]

    def slot(i):
        return pl.ds(pl.multiple_of(lax.rem(i, SLOTS) * COLS, COLS), COLS)

    def load_g(i):
        n, c = place_of(i // units, lax.rem(i, units))
        columns = pl.ds(pl.multiple_of(c * COLS, COLS), COLS)
        return pltpu.make_async_copy(g_hbm.at[0, n, :, columns], g_v.at[:, slot(i)], g_sem.at[lax.rem(i, SLOTS)])

    def send(s, w, part=()):
        n, c = place_of(s, w)
        block = sums.at[(n, c, *part)]
        to = right + lax.rem(w, 2) * (left - right)
        return pltpu.make_async_remote_copy(
            src_ref=block,
            dst_ref=block,
            send_sem=send_sem.at[s, w],
            recv_sem=recv_sem.at[s, w],
            device_id={"dp": to},
            device_id_type=pl.DeviceIdType.MESH,
        )

    def arrived(s, w):
        n, c = place_of(s + 1, w)
        pltpu.make_async_copy(sums.at[n, c], sums.at[n, c], recv_sem.at[s, w]).wait()

    def free(i):
        old = i - (ranks - 2) * units + 1

        @pl.when(jnp.logical_and(old >= 0, old < (ranks - 1) * units))
        def _():
            send(old // units, lax.rem(old, units)).wait_send()

    for h in range(SHARES):
        for copy in load_start(h):
            copy.start()

    greet(ranks)

    def term_of(n, some, top, bottom, columns):
        return lax.dot_general(
            a_v[n, some, top:bottom],
            g_v[some, columns],
            (((0,), (0,)), ((), ())),
            preferred_element_type=jnp.float32,
        )

    both = slice(0, 2 * COLS)
    for k in range(len(cuts) - 1):
        part = pl.ds(cuts[k], cuts[k + 1] - cuts[k])
        if k == 0:
            term = 0.0
            for h in range(SHARES):
                for copy in load_start(h):
                    copy.wait()
                if h == 0:
                    for later in range(1, len(cuts) - 1):
                        load_a0(later).start()
                    load_g(2).start()
                term += term_of(0, share(h), 0, FIRST, both)
        else:
            load_a0(k).wait()
            term = term_of(0, slice(None), cuts[k], cuts[k + 1], both)
        for i in range(2):
            n, c = place_of(0, i)
            sums[n, c, part] = term[:, i * COLS : (i + 1) * COLS].astype(sums.dtype)
            send(0, i, (part,)).start()
        if k == 0:
            load_a(1).start()
            load_g(3).start()
    load_g(4).start()
    load_g(5).start()

    def item(i, own):
        s, w = i // units, lax.rem(i, units)
        n = w // per_mat

        if own:

            @pl.when(lax.rem(w, per_mat) == 0)
            def _():
                load_a(n).wait()

            @pl.when(jnp.logical_and(lax.rem(w, per_mat) == 0, n + 1 < mats))
            def _():
                load_a(n + 1).start()

        load_g(i).wait()
        if not own:
            arrived(s - 1, w)
            free(i)
        n, c = place_of(s, w)
        for top in range(0, rows, ROWS):
            part = pl.ds(top, ROWS)
            term = term_of(n, slice(None), top, top + ROWS, slot(i))
            if not own:
                term += sums[n, c, part].astype(jnp.float32)
            sums[n, c, part] = term.astype(sums.dtype)
            send(s, w, (part,)).start()

        @pl.when(i + SLOTS < ranks * units)
        def _():
            load_g(i + SLOTS).start()

    def first_item(i, carry):
        item(i, True)
        return carry

    def later_item(i, carry):
        item(i, False)
        return carry

    def forward(j, carry):
        s, w = j // units, lax.rem(j, units)
        arrived(s - 1, w)
        free(j)
        send(s, w).start()
        return carry

    def finish(j, carry):
        s, w = j // units, lax.rem(j, units)
        send(s, w).wait_send()
        return carry

    def last(j, carry):
        arrived(j // units, lax.rem(j, units))
        return carry

    lax.fori_loop(2, units, first_item, 0)
    lax.fori_loop(units, ranks * units, later_item, 0)
    lax.fori_loop(ranks * units, end, forward, 0)
    lax.fori_loop(end - units, end, last, 0)
    lax.fori_loop((ranks - 1) * units, end, finish, 0)


def tail_kernel(ranks, sums, written, tail, send_sem, recv_sem):
    del written
    mats, blocks = sums.shape[:2]
    per_mat = blocks // ranks
    units = mats * per_mat
    me = lax.axis_index("dp")
    right = lax.rem(me + 1, ranks)
    left = lax.rem(me + ranks - 1, ranks)

    def send(w):
        n, c = place(ranks, per_mat, me, 2 * ranks - 3, w)
        t = w - (units - TAIL)
        return pltpu.make_async_remote_copy(
            src_ref=sums.at[n, c],
            dst_ref=tail.at[t],
            send_sem=send_sem.at[t],
            recv_sem=recv_sem.at[t],
            device_id={"dp": right + lax.rem(w, 2) * (left - right)},
            device_id_type=pl.DeviceIdType.MESH,
        )

    def start(w, carry):
        send(w).start()
        return carry

    def finish(w, carry):
        send(w).wait()
        return carry

    greet(ranks)
    lax.fori_loop(kept(units), units, start, 0)
    lax.fori_loop(kept(units), units, finish, 0)


def write_kernel(ranks, sums, out, sem):
    mats, blocks = sums.shape[:2]
    per_mat = blocks // ranks
    units = mats * per_mat
    me = lax.axis_index("dp")

    def copies(act):
        for w in range(units):
            for s in range(ranks):
                n, c = place(ranks, per_mat, me, s, w)
                columns = pl.ds(pl.multiple_of(c * COLS, COLS), COLS)
                copy = pltpu.make_async_copy(sums.at[n, c], out.at[n, :, columns], sem.at[w, s])
                if s == ranks - 2 and w >= units - TAIL:
                    pl.when(w < kept(units))(functools.partial(act, copy))
                else:
                    act(copy)

    copies(lambda copy: copy.start())
    copies(lambda copy: copy.wait())


def rest_kernel(ranks, per_mat, units, written, tail, out, sem):
    del written
    me = lax.axis_index("dp")

    def copies(act):
        for t in range(TAIL):
            w = units - TAIL + t
            n, c = place(ranks, per_mat, me, ranks - 2, w)
            columns = pl.ds(pl.multiple_of(c * COLS, COLS), COLS)
            copy = pltpu.make_async_copy(tail.at[t], out.at[n, :, columns], sem.at[t])
            pl.when(w >= kept(units))(functools.partial(act, copy))

    copies(lambda copy: copy.start())
    copies(lambda copy: copy.wait())


def solution(mesh):
    ranks = mesh.shape["dp"]

    def local(a, g):
        _, mats, tokens, rows = a.shape
        width = g.shape[-1]
        blocks = width // COLS
        units = blocks // ranks * mats
        phases = 2 * ranks - 2
        sums = pl.pallas_call(
            functools.partial(ring_kernel, ranks),
            out_shape=pltpu.VMEM((mats, blocks, rows, COLS), jnp.bfloat16),
            in_specs=[pl.BlockSpec(memory_space=pltpu.HBM)] * 2,
            out_specs=pl.BlockSpec(memory_space=pltpu.VMEM),
            scratch_shapes=[
                pltpu.VMEM((mats, tokens, rows), jnp.bfloat16),
                pltpu.VMEM((tokens, SLOTS * COLS), jnp.bfloat16),
                pltpu.SemaphoreType.DMA((mats,)),
                pltpu.SemaphoreType.DMA((1 + rows // ROWS,)),
                pltpu.SemaphoreType.DMA((SLOTS,)),
                pltpu.SemaphoreType.DMA((SHARES, 3)),
                pltpu.SemaphoreType.DMA((phases, units)),
                pltpu.SemaphoreType.DMA((phases, units)),
            ],
            compiler_params=pltpu.CompilerParams(
                collective_id=0, has_side_effects=True, vmem_limit_bytes=44 * 2**20
            ),
            name="ring",
        )(a, g)
        sums = pltpu.with_memory_space_constraint(sums, pltpu.VMEM)
        hbm, vmem = pl.BlockSpec(memory_space=pltpu.HBM), pl.BlockSpec(memory_space=pltpu.VMEM)
        whole = jax.ShapeDtypeStruct((mats, rows, width), jnp.bfloat16)
        written = pl.pallas_call(
            functools.partial(write_kernel, ranks),
            out_shape=whole,
            in_specs=[vmem],
            out_specs=hbm,
            scratch_shapes=[pltpu.SemaphoreType.DMA((units, ranks))],
            compiler_params=pltpu.CompilerParams(vmem_limit_bytes=2**20),
            name="write",
        )(sums)
        tail = pl.pallas_call(
            functools.partial(tail_kernel, ranks),
            out_shape=pltpu.VMEM((TAIL, rows, COLS), jnp.bfloat16),
            in_specs=[vmem, hbm],
            out_specs=vmem,
            scratch_shapes=[pltpu.SemaphoreType.DMA((TAIL,))] * 2,
            compiler_params=pltpu.CompilerParams(
                collective_id=1, has_side_effects=True, vmem_limit_bytes=2**20
            ),
            name="tail",
        )(sums, pltpu.with_memory_space_constraint(written, pltpu.HBM))
        return pl.pallas_call(
            functools.partial(rest_kernel, ranks, blocks // ranks, units),
            out_shape=whole,
            in_specs=[hbm, vmem],
            out_specs=hbm,
            input_output_aliases={0: 0},
            scratch_shapes=[pltpu.SemaphoreType.DMA((TAIL,))],
            compiler_params=pltpu.CompilerParams(vmem_limit_bytes=2**20),
            name="rest",
        )(written, pltpu.with_memory_space_constraint(tail, pltpu.VMEM))

    return jax.shard_map(
        local, mesh=mesh, in_specs=P(("rep", "dp")), out_specs=P("rep"), check_vma=False
    )
```

```python
import functools

import jax
import jax.numpy as jnp
from jax import lax
from jax.experimental import pallas as pl
from jax.experimental.pallas import tpu as pltpu
from jax.sharding import PartitionSpec as P

COLS = 256
ROWS = 256
FIRST = 128
SHARES = 8
TAIL, LAST = 8, 2
SLOTS = 4


def place(ranks, per_mat, me, s, w):
    to_left = lax.rem(w, 2)
    b = lax.rem(me + 2 * ranks - s + to_left * (2 * s), ranks)
    return w // per_mat, lax.rem(w, per_mat) * ranks + b


def columns_of(c):
    return pl.ds(pl.multiple_of(c * COLS, COLS), COLS)


def kept(units):
    return units - LAST - lax.rem(lax.axis_index("rep"), 2) * (TAIL - LAST)


def greet(ranks):
    me = lax.axis_index("dp")
    right = lax.rem(me + 1, ranks)
    left = lax.rem(me + ranks - 1, ranks)
    barrier = pltpu.get_barrier_semaphore()
    for neighbour in (left, right):
        pl.semaphore_signal(barrier, inc=1, device_id={"dp": neighbour}, device_id_type=pl.DeviceIdType.MESH)
    pl.semaphore_wait(barrier, 2)


def ring_kernel(ranks, a_hbm, g_hbm, sums, a_v, g_v, a_sem, a0_sem, g_sem, start_sem, send_sem, recv_sem):
    mats, rows, width = sums.shape
    per_mat = width // COLS // ranks
    units = mats * per_mat
    me = lax.axis_index("dp")
    right = lax.rem(me + 1, ranks)
    left = lax.rem(me + ranks - 1, ranks)

    end = (2 * ranks - 3) * units + kept(units)

    def place_of(s, w):
        return place(ranks, per_mat, me, s, w)

    def load_a(n):
        return pltpu.make_async_copy(a_hbm.at[0, n], a_v.at[n], a_sem.at[n])

    cuts = [0, FIRST, *range(ROWS, rows + 1, ROWS)]
    tokens = a_v.shape[1]

    def load_a0(k):
        columns = pl.ds(cuts[k], cuts[k + 1] - cuts[k])
        return pltpu.make_async_copy(a_hbm.at[0, 0, :, columns], a_v.at[0, :, columns], a0_sem.at[k])

    def share(h):
        return pl.ds(h * (tokens // SHARES), tokens // SHARES)

    def load_start(h):
        some = share(h)
        copies = [(a_hbm.at[0, 0, some, pl.ds(0, FIRST)], a_v.at[0, some, pl.ds(0, FIRST)])]
        for i in range(2):
            n, c = place_of(0, i)
            columns = pl.ds(pl.multiple_of(c * COLS, COLS), COLS)
            copies.append((g_hbm.at[0, n, some, columns], g_v.at[some, pl.ds(i * COLS, COLS)]))
        return [pltpu.make_async_copy(*copy, start_sem.at[h, k]) for k, copy in enumerate(copies)]

    def slot(i):
        return pl.ds(pl.multiple_of(lax.rem(i, SLOTS) * COLS, COLS), COLS)

    def load_g(i):
        n, c = place_of(i // units, lax.rem(i, units))
        columns = pl.ds(pl.multiple_of(c * COLS, COLS), COLS)
        return pltpu.make_async_copy(g_hbm.at[0, n, :, columns], g_v.at[:, slot(i)], g_sem.at[lax.rem(i, SLOTS)])

    def send(s, w, part=slice(None)):
        n, c = place_of(s, w)
        block = sums.at[n, part, columns_of(c)]
        to = right + lax.rem(w, 2) * (left - right)
        return pltpu.make_async_remote_copy(
            src_ref=block,
            dst_ref=block,
            send_sem=send_sem.at[s, w],
            recv_sem=recv_sem.at[s, w],
            device_id={"dp": to},
            device_id_type=pl.DeviceIdType.MESH,
        )

    def arrived(s, w):
        n, c = place_of(s + 1, w)
        block = sums.at[n, :, columns_of(c)]
        pltpu.make_async_copy(block, block, recv_sem.at[s, w]).wait()

    def free(i):
        old = i - (ranks - 2) * units + 1

        @pl.when(jnp.logical_and(old >= 0, old < (ranks - 1) * units))
        def _():
            send(old // units, lax.rem(old, units)).wait_send()

    for h in range(SHARES):
        for copy in load_start(h):
            copy.start()

    greet(ranks)

    def term_of(n, some, top, bottom, columns):
        return lax.dot_general(
            a_v[n, some, top:bottom],
            g_v[some, columns],
            (((0,), (0,)), ((), ())),
            preferred_element_type=jnp.float32,
        )

    both = slice(0, 2 * COLS)
    for k in range(len(cuts) - 1):
        part = pl.ds(cuts[k], cuts[k + 1] - cuts[k])
        if k == 0:
            term = 0.0
            for h in range(SHARES):
                for copy in load_start(h):
                    copy.wait()
                if h == 0:
                    for later in range(1, len(cuts) - 1):
                        load_a0(later).start()
                    load_g(2).start()
                term += term_of(0, share(h), 0, FIRST, both)
        else:
            load_a0(k).wait()
            term = term_of(0, slice(None), cuts[k], cuts[k + 1], both)
        for i in range(2):
            n, c = place_of(0, i)
            sums[n, part, columns_of(c)] = term[:, i * COLS : (i + 1) * COLS].astype(sums.dtype)
            send(0, i, part).start()
        if k == 0:
            load_a(1).start()
            load_g(3).start()
    load_g(4).start()
    load_g(5).start()

    def item(i, own):
        s, w = i // units, lax.rem(i, units)
        n = w // per_mat

        if own:

            @pl.when(lax.rem(w, per_mat) == 0)
            def _():
                load_a(n).wait()

            @pl.when(jnp.logical_and(lax.rem(w, per_mat) == 0, n + 1 < mats))
            def _():
                load_a(n + 1).start()

        load_g(i).wait()
        if not own:
            arrived(s - 1, w)
            free(i)
        n, c = place_of(s, w)
        for top in range(0, rows, ROWS):
            part = pl.ds(top, ROWS)
            term = term_of(n, slice(None), top, top + ROWS, slot(i))
            if not own:
                term += sums[n, part, columns_of(c)].astype(jnp.float32)
            sums[n, part, columns_of(c)] = term.astype(sums.dtype)
            send(s, w, part).start()

        @pl.when(i + SLOTS < ranks * units)
        def _():
            load_g(i + SLOTS).start()

    def first_item(i, carry):
        item(i, True)
        return carry

    def later_item(i, carry):
        item(i, False)
        return carry

    def forward(j, carry):
        s, w = j // units, lax.rem(j, units)
        arrived(s - 1, w)
        free(j)
        send(s, w).start()
        return carry

    def finish(j, carry):
        s, w = j // units, lax.rem(j, units)
        send(s, w).wait_send()
        return carry

    def last(j, carry):
        arrived(j // units, lax.rem(j, units))
        return carry

    lax.fori_loop(2, units, first_item, 0)
    lax.fori_loop(units, ranks * units, later_item, 0)
    lax.fori_loop(ranks * units, end, forward, 0)
    lax.fori_loop(end - units, end, last, 0)
    lax.fori_loop((ranks - 1) * units, end, finish, 0)


def tail_kernel(ranks, sums, written, tail, send_sem, recv_sem):
    del written
    mats, _, width = sums.shape
    per_mat = width // COLS // ranks
    units = mats * per_mat
    me = lax.axis_index("dp")
    right = lax.rem(me + 1, ranks)
    left = lax.rem(me + ranks - 1, ranks)

    def send(w):
        n, c = place(ranks, per_mat, me, 2 * ranks - 3, w)
        t = w - (units - TAIL)
        return pltpu.make_async_remote_copy(
            src_ref=sums.at[n, :, columns_of(c)],
            dst_ref=tail.at[t],
            send_sem=send_sem.at[t],
            recv_sem=recv_sem.at[t],
            device_id={"dp": right + lax.rem(w, 2) * (left - right)},
            device_id_type=pl.DeviceIdType.MESH,
        )

    def start(w, carry):
        send(w).start()
        return carry

    def finish(w, carry):
        send(w).wait()
        return carry

    greet(ranks)
    lax.fori_loop(kept(units), units, start, 0)
    lax.fori_loop(kept(units), units, finish, 0)


def write_kernel(sums, out, sem):
    mats, rows, _ = sums.shape

    def copies(act):
        for n in range(mats):
            for k in range(rows // FIRST):
                part = pl.ds(k * FIRST, FIRST)
                act(pltpu.make_async_copy(sums.at[n, part], out.at[n, part], sem.at[n, k]))

    copies(lambda copy: copy.start())
    copies(lambda copy: copy.wait())


def rest_kernel(ranks, per_mat, units, written, tail, out, sem):
    del written
    me = lax.axis_index("dp")

    def copies(act):
        for t in range(TAIL):
            w = units - TAIL + t
            n, c = place(ranks, per_mat, me, ranks - 2, w)
            columns = pl.ds(pl.multiple_of(c * COLS, COLS), COLS)
            copy = pltpu.make_async_copy(tail.at[t], out.at[n, :, columns], sem.at[t])
            pl.when(w >= kept(units))(functools.partial(act, copy))

    copies(lambda copy: copy.start())
    copies(lambda copy: copy.wait())


def solution(mesh):
    ranks = mesh.shape["dp"]

    def local(a, g):
        _, mats, tokens, rows = a.shape
        width = g.shape[-1]
        blocks = width // COLS
        units = blocks // ranks * mats
        phases = 2 * ranks - 2
        sums = pl.pallas_call(
            functools.partial(ring_kernel, ranks),
            out_shape=pltpu.VMEM((mats, rows, width), jnp.bfloat16),
            in_specs=[pl.BlockSpec(memory_space=pltpu.HBM)] * 2,
            out_specs=pl.BlockSpec(memory_space=pltpu.VMEM),
            scratch_shapes=[
                pltpu.VMEM((mats, tokens, rows), jnp.bfloat16),
                pltpu.VMEM((tokens, SLOTS * COLS), jnp.bfloat16),
                pltpu.SemaphoreType.DMA((mats,)),
                pltpu.SemaphoreType.DMA((1 + rows // ROWS,)),
                pltpu.SemaphoreType.DMA((SLOTS,)),
                pltpu.SemaphoreType.DMA((SHARES, 3)),
                pltpu.SemaphoreType.DMA((phases, units)),
                pltpu.SemaphoreType.DMA((phases, units)),
            ],
            compiler_params=pltpu.CompilerParams(
                collective_id=0, has_side_effects=True, vmem_limit_bytes=44 * 2**20
            ),
            name="ring",
        )(a, g)
        sums = pltpu.with_memory_space_constraint(sums, pltpu.VMEM)
        hbm, vmem = pl.BlockSpec(memory_space=pltpu.HBM), pl.BlockSpec(memory_space=pltpu.VMEM)
        whole = jax.ShapeDtypeStruct((mats, rows, width), jnp.bfloat16)
        written = pl.pallas_call(
            write_kernel,
            out_shape=whole,
            in_specs=[vmem],
            out_specs=hbm,
            scratch_shapes=[pltpu.SemaphoreType.DMA((mats, rows // FIRST))],
            compiler_params=pltpu.CompilerParams(vmem_limit_bytes=2**20),
            name="write",
        )(sums)
        tail = pl.pallas_call(
            functools.partial(tail_kernel, ranks),
            out_shape=pltpu.VMEM((TAIL, rows, COLS), jnp.bfloat16),
            in_specs=[vmem, hbm],
            out_specs=vmem,
            scratch_shapes=[pltpu.SemaphoreType.DMA((TAIL,))] * 2,
            compiler_params=pltpu.CompilerParams(
                collective_id=1, has_side_effects=True, vmem_limit_bytes=2**20
            ),
            name="tail",
        )(sums, pltpu.with_memory_space_constraint(written, pltpu.HBM))
        return pl.pallas_call(
            functools.partial(rest_kernel, ranks, blocks // ranks, units),
            out_shape=whole,
            in_specs=[hbm, vmem],
            out_specs=hbm,
            input_output_aliases={0: 0},
            scratch_shapes=[pltpu.SemaphoreType.DMA((TAIL,))],
            compiler_params=pltpu.CompilerParams(vmem_limit_bytes=2**20),
            name="rest",
        )(written, pltpu.with_memory_space_constraint(tail, pltpu.VMEM))

    return jax.shard_map(
        local, mesh=mesh, in_specs=P(("rep", "dp")), out_specs=P("rep"), check_vma=False
    )
```
